32 devices in a mesh: grp: 4 (over x, core), dp: 8 (over z, y).
Axes of the slice: x: 2, y: 2, z: 4, core: 2. Of those that a mesh axis runs over, the one named last changes fastest.
Arguments:
- gradients: bfloat16 [4, 8, 16384, 128], P('grp', 'dp'), may hold values from -48 to 48
- block_len: int32 [16], replicated, may hold values from 1 to 524288, 2097152 in all
- amax_history: float32 [4, 16], replicated, may hold values from 20 to 200
Outputs:
- mean_grad: bfloat16 [16384, 128], P('dp')
- block_amax: bfloat16 [16], replicated
The draws below stay inside these ranges and needn't reach their ends.
Inputs may be any that keep to these rules, and one draw needn't show every extreme that they name: `block_len`: every tensor has at least one entry; the lengths sum to 2097152.
All inputs are finite; a program needn't handle non-finite values.
Results may differ from the reference program's by a relative error of at most 0.018.
Values may be sent and summed in bfloat16 or wider, within the bound.
A program may use at most 64 MiB of HBM per device.

```python
import math
import jax
import jax.numpy as jnp
import numpy as np
from jax import lax

ROWS = 16384
BLOCKS = 16
HIST = 4
N_GRP = 4
N_DP = 8
DEVICES = 32


def block_scale(own_key, dims, cuts, least, largest):
    factor_of = 1.0
    for dim, shards_of in cuts:
        draws = jax.random.uniform(jax.random.fold_in(jax.random.fold_in(own_key, 6), dim), (shards_of,), jnp.float32, least / len(cuts), largest / len(cuts))
        factor_of = factor_of * jnp.repeat(jnp.exp(draws), dims[dim] // shards_of).reshape((-1,) + (1,) * (len(dims) - 1 - dim))
    return factor_of


def split_up(count, total, most, lean):
    weights = [(1 << 20) // math.isqrt(rank ** lean) + 1 for rank in range(2, count + 1)]
    surplus, counts = total - most - (count - 1), [1] * (count - 1)
    while surplus > 0:
        candidates = [i for i in range(count - 1) if counts[i] < most]
        mass, budget = sum([weights[i] for i in candidates]), surplus
        for i in candidates:
            extra = min(most - counts[i], max(1, budget * weights[i] // mass), surplus)
            counts[i] = counts[i] + extra
            surplus = surplus - extra
    return np.array([most] + counts)


def uneven(own_key, amount, total, bound, skew):
    if amount == 2:
        one = jax.random.randint(own_key, (), max(1, total - bound), min(bound, total - 1) + 1)
        return jnp.stack([one, total - one])
    lengths = jnp.asarray(split_up(amount, total, bound, skew), jnp.int32)
    couples = (amount - 1) // 2
    giver, sink = lengths[1:1 + 2 * couples:2], lengths[2:2 + 2 * couples:2]
    slack = jnp.minimum(giver - 1, bound - sink)
    passed = jax.random.randint(jax.random.fold_in(own_key, 1), (couples,), 0, 1 << 20) % (slack + 1)
    lengths = lengths.at[1:1 + 2 * couples:2].set(giver - passed).at[2:2 + 2 * couples:2].set(sink + passed)
    return lengths[jax.random.permutation(jax.random.fold_in(own_key, 2), amount)]


def noise(rng, extent, spread, most, shards=(), held_as=jnp.bfloat16):
    entries = spread * jax.random.normal(rng, extent, jnp.float32)
    if shards:
        entries = entries * block_scale(rng, extent, shards, -0.22, 0.18)
    return jnp.clip(entries, -most, most).astype(held_as)


def setup_inputs(seed: int = 0) -> dict:
    key_list = jax.random.split(jax.random.key(seed), 4)
    return {
        "gradients": noise(key_list[0], (N_GRP, N_DP, ROWS, 128), 8.0, 48.0, ((0, 4), (1, 8))),
        "block_len": uneven(key_list[1], BLOCKS, ROWS * 128, ROWS * 32, 2).astype(jnp.int32),
        "amax_history": jnp.clip(jnp.exp(jax.random.uniform(key_list[2], (HIST, BLOCKS), jnp.float32, math.log(20.0), math.log(200.0))), 20.0, 200.0),
    }


SATURATE = 448.0


def reference(gradients, block_len, amax_history):
    block_ends = jnp.cumsum(block_len).astype(jnp.int32)
    position = (jnp.arange(ROWS, dtype=jnp.int32)[:, None] * 128 + jnp.arange(128, dtype=jnp.int32)[None, :])
    block = jnp.sum((position[:, :, None] >= block_ends[None, None, :]).astype(jnp.int32), axis=-1)
    in_block = block[:, :, None] == jnp.arange(BLOCKS, dtype=jnp.int32)[None, None, :]
    scales = SATURATE / jnp.maximum(jnp.max(amax_history, axis=0), 1.0)
    scale_elem = jnp.sum(jnp.where(in_block, scales[None, None, :], jnp.float32(0.0)), axis=-1)

    def one_group(carry, group_grads):
        accumulated, maxima = carry
        summed = jnp.sum(group_grads.astype(jnp.float32), axis=0)
        local_max = jnp.max(jnp.where(in_block, jnp.abs(summed)[:, :, None], jnp.float32(0.0)), axis=(0, 1))
        quantized = jnp.clip(summed * scale_elem, -SATURATE, SATURATE).astype(jnp.bfloat16)
        return (accumulated + quantized.astype(jnp.float32), jnp.maximum(maxima, local_max)), None

    start = (jnp.zeros((ROWS, 128), jnp.float32), jnp.zeros((BLOCKS,), jnp.float32))
    (accumulated, maxima), unused = lax.scan(one_group, start, gradients)
    mean_grad = (accumulated / scale_elem / DEVICES).astype(jnp.bfloat16)
    return mean_grad, maxima.astype(jnp.bfloat16)
```

```python
import functools

import jax
import jax.numpy as jnp
from jax import lax
from jax.experimental import pallas as pl
from jax.experimental.pallas import tpu as pltpu
from jax.sharding import PartitionSpec as P

SATURATE = 448.0
CHUNKS = 8
CORES = 2
MESH = pl.DeviceIdType.MESH


def y_extent(dp):
    y = 1
    while (2 * y) * (2 * y) <= dp:
        y *= 2
    return y


def kernel(
    cfg, len_ref, hist_ref, grad, out, amax_out,
    own, ybuf, part, zbuf, q, cbuf, xbuf, scale_buf, svec, acc, msg, dpmax, grpmsg, grpmax,
    own_sem, y_send, y_recv, z_send, z_recv, c_send, c_recv, x_send, x_recv,
    o_send, o_recv, dm_send, dm_recv, gm_send, gm_recv,
):
    dp, grp, Y, Z, X, K, H, piece = cfg
    blocks = len_ref.shape[0]
    hist = hist_ref.shape[0]
    d = lax.axis_index("dp")
    g = lax.axis_index("grp")
    z, y = d // Y, d % Y
    x, core = g // CORES, g % CORES
    sibling = x * CORES + (1 - core)
    lines = CORES * H
    base = d * (K * lines)

    def copy(src, dst, send, recv, target):
        return pltpu.make_async_remote_copy(
            src_ref=src, dst_ref=dst, send_sem=send, recv_sem=recv,
            device_id=target, device_id_type=MESH,
        )

    def own_copy(k):
        return pltpu.make_async_copy(grad.at[:, y, k], own.at[k], own_sem.at[k])

    def y_copy(k, j):
        peer = (y + j) % Y
        return copy(grad.at[:, peer, k], ybuf.at[k, j - 1], y_send.at[k, j - 1],
                    y_recv.at[k, j - 1], {"dp": z * Y + peer})

    def z_copy(k, j):
        peer = (z + j) % Z
        return copy(part.at[k, j - 1], zbuf.at[k, j - 1], z_send.at[k, j - 1],
                    z_recv.at[k, j - 1], {"dp": peer * Y + y})

    def c_copy(k):
        return copy(q.at[k, 1 - core], cbuf.at[k], c_send.at[k], c_recv.at[k],
                    {"grp": sibling})

    def x_copy(k, j):
        peer = (x + j) % X
        return copy(xbuf.at[k, x], xbuf.at[k, x], x_send.at[k, j - 1], x_recv.at[k, j - 1],
                    {"grp": peer * CORES + core})

    def x_arrival(k, j):
        peer = (x + X - j) % X
        return copy(xbuf.at[k, peer], xbuf.at[k, peer], x_send.at[k, j - 1],
                    x_recv.at[k, j - 1], {"grp": peer * CORES + core})

    def o_copy(k):
        return copy(out.at[k, core], out.at[k, core], o_send.at[k], o_recv.at[k],
                    {"grp": sibling})

    def o_arrival(k):
        return copy(out.at[k, 1 - core], out.at[k, 1 - core], o_send.at[k], o_recv.at[k],
                    {"grp": sibling})

    def dm_copy(j):
        return copy(msg, dpmax.at[j - 1], dm_send.at[j - 1], dm_recv.at[j - 1],
                    {"dp": (d + j) % dp})

    def gm_copy(j):
        return copy(grpmsg, grpmax.at[j - 1], gm_send.at[j - 1], gm_recv.at[j - 1],
                    {"grp": (g + j) % grp})

    barrier = pltpu.get_barrier_semaphore()
    for j in range(1, dp):
        pl.semaphore_signal(barrier, inc=1, device_id={"dp": (d + j) % dp}, device_id_type=MESH)
    for j in range(1, grp):
        pl.semaphore_signal(barrier, inc=1, device_id={"grp": (g + j) % grp}, device_id_type=MESH)

    def load(k, carry):
        own_copy(k).start()
        return carry

    lax.fori_loop(0, K, load, 0)
    ends = []
    total = jnp.int32(0)
    for c in range(blocks):
        total = total + len_ref[c]
        ends.append(total)
        top = jnp.full((8, 128), hist_ref[0, c], jnp.float32)
        for h in range(1, hist):
            top = jnp.maximum(top, jnp.full((8, 128), hist_ref[h, c], jnp.float32))
        svec[c] = SATURATE / jnp.maximum(top, 1.0)
    acc[...] = jnp.zeros(acc.shape, jnp.float32)
    pl.semaphore_wait(barrier, dp - 1 + grp - 1)

    def send_y(k, carry):
        for j in range(1, Y):
            y_copy(k, j).start()
        return carry

    lax.fori_loop(0, K, send_y, 0)

    def stage_z(k):
        own_copy(k).wait()
        for j in range(1, Y):
            y_copy(k, j).wait_recv()
        for j in range(1, Z):
            peer = (z + j) % Z
            value = own[k, peer].astype(jnp.float32)
            for i in range(Y - 1):
                value = value + ybuf[k, i, peer].astype(jnp.float32)
            part[k, j - 1] = value.astype(jnp.bfloat16)
            z_copy(k, j).start()

    def stage_q(k):
        for j in range(1, Z):
            z_copy(k, j).wait_recv()
        for half in range(CORES):
            def step(i, tops):
                rows = pl.ds(pl.multiple_of(i * piece, piece), piece)
                value = own[k, z, half, rows].astype(jnp.float32)
                for a in range(Y - 1):
                    value = value + ybuf[k, a, z, half, rows].astype(jnp.float32)
                for a in range(Z - 1):
                    value = value + zbuf[k, a, half, rows].astype(jnp.float32)
                value = value.reshape(piece // 8, 8, 128)
                shape = value.shape
                first = (base + k * lines + half * H + i * piece) * 128
                place = (
                    lax.broadcasted_iota(jnp.int32, shape, 0) * 1024
                    + lax.broadcasted_iota(jnp.int32, shape, 1) * 128
                    + lax.broadcasted_iota(jnp.int32, shape, 2)
                ) + first
                size = jnp.abs(value)
                scale = jnp.broadcast_to(svec[0][None], shape)
                below = place < ends[0]
                new = [jnp.maximum(tops[0], jnp.max(jnp.where(below, size, 0.0), axis=0))]
                for c in range(1, blocks):
                    after = place >= ends[c - 1]
                    scale = jnp.where(after, svec[c][None], scale)
                    inside = after & (place < ends[c])
                    new.append(jnp.maximum(tops[c], jnp.max(jnp.where(inside, size, 0.0), axis=0)))
                scale_buf[k, half, rows] = scale.reshape(piece, 128)
                quant = jnp.clip(value * scale, -SATURATE, SATURATE)
                q[k, half, rows] = quant.reshape(piece, 128).astype(jnp.bfloat16)
                return tuple(new)

            tops = lax.fori_loop(0, H // piece, step, tuple(acc[c] for c in range(blocks)))
            for c in range(blocks):
                acc[c] = tops[c]
        c_copy(k).start()

    def stage_max():
        top = jnp.max(acc[...], axis=1)
        top = jnp.max(top, axis=1, keepdims=True)
        lane = lax.broadcasted_iota(jnp.int32, (blocks, 128), 1)
        row = lax.broadcasted_iota(jnp.int32, (blocks, 128), 0)
        flat = jnp.max(jnp.where(lane == row, top, 0.0), axis=0, keepdims=True)
        msg[...] = jnp.broadcast_to(flat, msg.shape)
        for j in range(1, dp):
            dm_copy(j).start()

    def stage_x(k):
        c_copy(k).wait_recv()
        both = q[k, core].astype(jnp.float32) + cbuf[k].astype(jnp.float32)
        xbuf[k, x] = both.astype(jnp.bfloat16)
        for j in range(1, X):
            x_copy(k, j).start()

    def stage_out(k):
        for j in range(1, X):
            x_arrival(k, j).wait_recv()
        value = xbuf[k, 0].astype(jnp.float32)
        for a in range(1, X):
            value = value + xbuf[k, a].astype(jnp.float32)
        mean = value / scale_buf[k, core] / (dp * grp)
        out[k, core] = mean.astype(jnp.bfloat16)
        o_copy(k).start()

    stages = ((stage_z, 0), (stage_q, 2), (stage_x, 3), (stage_out, 4))

    def tick(t, carry):
        for stage, delay in stages:
            @pl.when((t >= delay) & (t < K + delay))
            def _(stage=stage, delay=delay):
                stage(t - delay)

            if stage is stage_q:
                @pl.when(t == K - 1 + delay)
                def _():
                    stage_max()
        return carry

    lax.fori_loop(0, K + 4, tick, 0)

    for j in range(1, dp):
        dm_copy(j).wait_recv()
    top = msg[...]
    for j in range(1, dp):
        top = jnp.maximum(top, dpmax[j - 1])
    grpmsg[...] = top
    for j in range(1, grp):
        gm_copy(j).start()
    for j in range(1, grp):
        gm_copy(j).wait_recv()
    for j in range(1, grp):
        top = jnp.maximum(top, grpmax[j - 1])
    amax_out[...] = top

    def finish(k, carry):
        for j in range(1, Y):
            y_copy(k, j).wait_send()
        for j in range(1, Z):
            z_copy(k, j).wait_send()
        c_copy(k).wait_send()
        for j in range(1, X):
            x_copy(k, j).wait_send()
        o_copy(k).wait_send()
        o_arrival(k).wait_recv()
        return carry

    lax.fori_loop(0, K, finish, 0)
    for j in range(1, dp):
        dm_copy(j).wait_send()
    for j in range(1, grp):
        gm_copy(j).wait_send()


def body(gradients, block_len, amax_history):
    dp = lax.axis_size("dp")
    grp = lax.axis_size("grp")
    rows, lanes = gradients.shape[2:]
    Y = y_extent(dp)
    Z = dp // Y
    X = grp // CORES
    K = CHUNKS
    H = rows // dp // K // CORES
    piece = min(32, H)
    blocks = block_len.shape[0]
    cfg = (dp, grp, Y, Z, X, K, H, piece)
    bf, f32 = jnp.bfloat16, jnp.float32
    sem = pltpu.SemaphoreType.DMA
    tile = (CORES, H, lanes)
    scratch = [
        pltpu.VMEM((K, Z) + tile, bf),
        pltpu.VMEM((K, Y - 1, Z) + tile, bf),
        pltpu.VMEM((K, Z - 1) + tile, bf),
        pltpu.VMEM((K, Z - 1) + tile, bf),
        pltpu.VMEM((K,) + tile, bf),
        pltpu.VMEM((K, H, lanes), bf),
        pltpu.VMEM((K, X, H, lanes), bf),
        pltpu.VMEM((K,) + tile, f32),
        pltpu.VMEM((blocks, 8, lanes), f32),
        pltpu.VMEM((blocks, 8, lanes), f32),
        pltpu.VMEM((8, lanes), f32),
        pltpu.VMEM((dp - 1, 8, lanes), f32),
        pltpu.VMEM((8, lanes), f32),
        pltpu.VMEM((grp - 1, 8, lanes), f32),
        sem((K,)),
        sem((K, Y - 1)), sem((K, Y - 1)),
        sem((K, Z - 1)), sem((K, Z - 1)),
        sem((K,)), sem((K,)),
        sem((K, X - 1)), sem((K, X - 1)),
        sem((K,)), sem((K,)),
        sem((dp - 1,)), sem((dp - 1,)),
        sem((grp - 1,)), sem((grp - 1,)),
    ]
    mean, top = pl.pallas_call(
        functools.partial(kernel, cfg),
        out_shape=(
            jax.ShapeDtypeStruct((K,) + tile, bf),
            jax.ShapeDtypeStruct((8, lanes), f32),
        ),
        in_specs=[
            pl.BlockSpec(memory_space=pltpu.SMEM),
            pl.BlockSpec(memory_space=pltpu.SMEM),
            pl.BlockSpec(memory_space=pl.ANY),
        ],
        out_specs=(
            pl.BlockSpec(memory_space=pltpu.VMEM),
            pl.BlockSpec(memory_space=pltpu.VMEM),
        ),
        scratch_shapes=scratch,
        compiler_params=pltpu.CompilerParams(collective_id=0, has_side_effects=True),
    )(block_len, amax_history, gradients.reshape((Z, Y, K) + tile))
    return mean.reshape(rows // dp, lanes), top[0, :blocks].astype(bf)


def solution(mesh):
    placed = (P("grp", "dp", None, None), P(), P())
    return jax.shard_map(
        body, mesh=mesh, in_specs=placed, out_specs=(P("dp", None), P()), check_vma=False
    )
```

```python
import functools

import jax
import jax.numpy as jnp
from jax import lax
from jax.experimental import pallas as pl
from jax.experimental.pallas import tpu as pltpu
from jax.sharding import PartitionSpec as P

SATURATE = 448.0
CHUNKS = 16
DELAYS = (0, 3, 5)
MESH = pl.DeviceIdType.MESH


def y_extent(dp):
    y = 1
    while (2 * y) * (2 * y) <= dp:
        y *= 2
    return y


def kernel(
    cfg, len_ref, hist_ref, grad, out, amax_out,
    own, ybuf, part, zbuf, qbuf, scale_buf, svec, acc, msg, dpmax, grpmsg, grpmax,
    own_sem, y_send, y_recv, z_send, z_recv, q_send, q_recv,
    dm_send, dm_recv, gm_send, gm_recv,
):
    dp, grp, Y, Z, K, lines, piece = cfg
    blocks = len_ref.shape[0]
    hist = hist_ref.shape[0]
    d = lax.axis_index("dp")
    g = lax.axis_index("grp")
    z, y = d // Y, d % Y
    base = d * (K * lines)

    def copy(src, dst, send, recv, target):
        return pltpu.make_async_remote_copy(
            src_ref=src, dst_ref=dst, send_sem=send, recv_sem=recv,
            device_id=target, device_id_type=MESH,
        )

    def own_copy(k):
        return pltpu.make_async_copy(grad.at[:, y, k], own.at[k], own_sem.at[k])

    def y_copy(k, j):
        peer = (y + j) % Y
        return copy(grad.at[:, peer, k], ybuf.at[k, j - 1], y_send.at[k, j - 1],
                    y_recv.at[k, j - 1], {"dp": z * Y + peer})

    def z_copy(k, j):
        peer = (z + j) % Z
        return copy(part.at[k, j - 1], zbuf.at[k, j - 1], z_send.at[k, j - 1],
                    z_recv.at[k, j - 1], {"dp": peer * Y + y})

    def q_copy(k, j):
        return copy(qbuf.at[k, g], qbuf.at[k, g], q_send.at[k, j - 1], q_recv.at[k, j - 1],
                    {"grp": (g + j) % grp})

    def q_arrival(k, j):
        peer = (g + grp - j) % grp
        return copy(qbuf.at[k, peer], qbuf.at[k, peer], q_send.at[k, j - 1],
                    q_recv.at[k, j - 1], {"grp": peer})

    def dm_copy(j):
        return copy(msg, dpmax.at[j - 1], dm_send.at[j - 1], dm_recv.at[j - 1],
                    {"dp": (d + j) % dp})

    def gm_copy(j):
        return copy(grpmsg, grpmax.at[j - 1], gm_send.at[j - 1], gm_recv.at[j - 1],
                    {"grp": (g + j) % grp})

    barrier = pltpu.get_barrier_semaphore()
    for j in range(1, dp):
        pl.semaphore_signal(barrier, inc=1, device_id={"dp": (d + j) % dp}, device_id_type=MESH)
    for j in range(1, grp):
        pl.semaphore_signal(barrier, inc=1, device_id={"grp": (g + j) % grp}, device_id_type=MESH)

    def load(k, carry):
        own_copy(k).start()
        return carry

    lax.fori_loop(0, K, load, 0)
    ends = []
    total = jnp.int32(0)
    for c in range(blocks):
        total = total + len_ref[c]
        ends.append(total)
        top = jnp.full((8, 128), hist_ref[0, c], jnp.float32)
        for h in range(1, hist):
            top = jnp.maximum(top, jnp.full((8, 128), hist_ref[h, c], jnp.float32))
        svec[c] = SATURATE / jnp.maximum(top, 1.0)
    acc[...] = jnp.zeros(acc.shape, jnp.float32)
    pl.semaphore_wait(barrier, dp - 1 + grp - 1)

    def send_y(k, carry):
        for j in range(1, Y):
            y_copy(k, j).start()
        return carry

    lax.fori_loop(0, K, send_y, 0)

    def stage_z(k):
        own_copy(k).wait()
        for j in range(1, Y):
            y_copy(k, j).wait_recv()
        for j in range(1, Z):
            peer = (z + j) % Z
            value = own[k, peer].astype(jnp.float32)
            for i in range(Y - 1):
                value = value + ybuf[k, i, peer].astype(jnp.float32)
            part[k, j - 1] = value.astype(jnp.bfloat16)
            z_copy(k, j).start()

    def stage_q(k):
        for j in range(1, Z):
            z_copy(k, j).wait_recv()
        def step(i, tops):
            rows = pl.ds(pl.multiple_of(i * piece, piece), piece)
            value = own[k, z, rows].astype(jnp.float32)
            for a in range(Y - 1):
                value = value + ybuf[k, a, z, rows].astype(jnp.float32)
            for a in range(Z - 1):
                value = value + zbuf[k, a, rows].astype(jnp.float32)
            value = value.reshape(piece // 8, 8, 128)
            shape = value.shape
            first = (base + k * lines + i * piece) * 128
            place = (
                lax.broadcasted_iota(jnp.int32, shape, 0) * 1024
                + lax.broadcasted_iota(jnp.int32, shape, 1) * 128
                + lax.broadcasted_iota(jnp.int32, shape, 2)
            ) + first
            size = jnp.abs(value)
            scale = jnp.broadcast_to(svec[0][None], shape)
            below = place < ends[0]
            new = [jnp.maximum(tops[0], jnp.max(jnp.where(below, size, 0.0), axis=0))]
            for c in range(1, blocks):
                after = place >= ends[c - 1]
                scale = jnp.where(after, svec[c][None], scale)
                inside = after & (place < ends[c])
                new.append(jnp.maximum(tops[c], jnp.max(jnp.where(inside, size, 0.0), axis=0)))
            scale_buf[k, rows] = scale.reshape(piece, 128)
            quant = jnp.clip(value * scale, -SATURATE, SATURATE)
            qbuf[k, g, rows] = quant.reshape(piece, 128).astype(jnp.bfloat16)
            return tuple(new)

        tops = lax.fori_loop(0, lines // piece, step, tuple(acc[c] for c in range(blocks)))
        for c in range(blocks):
            acc[c] = tops[c]
        for j in range(1, grp):
            q_copy(k, j).start()

    def stage_max():
        top = jnp.max(acc[...], axis=1)
        top = jnp.max(top, axis=1, keepdims=True)
        lane = lax.broadcasted_iota(jnp.int32, (blocks, 128), 1)
        row = lax.broadcasted_iota(jnp.int32, (blocks, 128), 0)
        flat = jnp.max(jnp.where(lane == row, top, 0.0), axis=0, keepdims=True)
        msg[...] = jnp.broadcast_to(flat, msg.shape)
        for j in range(1, dp):
            dm_copy(j).start()

    def stage_out(k):
        for j in range(1, grp):
            q_arrival(k, j).wait_recv()
        value = qbuf[k, 0].astype(jnp.float32)
        for a in range(1, grp):
            value = value + qbuf[k, a].astype(jnp.float32)
        out[k] = (value / scale_buf[k] / (dp * grp)).astype(jnp.bfloat16)

    stages = tuple(zip((stage_z, stage_q, stage_out), DELAYS))

    def tick(t, carry):
        for stage, delay in stages:
            @pl.when((t >= delay) & (t < K + delay))
            def _(stage=stage, delay=delay):
                stage(t - delay)

            if stage is stage_q:
                @pl.when(t == K - 1 + delay)
                def _():
                    stage_max()
        return carry

    lax.fori_loop(0, K + DELAYS[-1], tick, 0)

    for j in range(1, dp):
        dm_copy(j).wait_recv()
    top = msg[...]
    for j in range(1, dp):
        top = jnp.maximum(top, dpmax[j - 1])
    grpmsg[...] = top
    for j in range(1, grp):
        gm_copy(j).start()
    for j in range(1, grp):
        gm_copy(j).wait_recv()
    for j in range(1, grp):
        top = jnp.maximum(top, grpmax[j - 1])
    amax_out[...] = top.astype(jnp.bfloat16)

    def finish(k, carry):
        for j in range(1, Y):
            y_copy(k, j).wait_send()
        for j in range(1, Z):
            z_copy(k, j).wait_send()
        for j in range(1, grp):
            q_copy(k, j).wait_send()
        return carry

    lax.fori_loop(0, K, finish, 0)
    for j in range(1, dp):
        dm_copy(j).wait_send()
    for j in range(1, grp):
        gm_copy(j).wait_send()


def body(gradients, block_len, amax_history):
    dp = lax.axis_size("dp")
    grp = lax.axis_size("grp")
    rows, lanes = gradients.shape[2:]
    Y = y_extent(dp)
    Z = dp // Y
    K = min(CHUNKS, rows // dp // 32)
    lines = rows // dp // K
    piece = 32
    blocks = block_len.shape[0]
    cfg = (dp, grp, Y, Z, K, lines, piece)
    bf, f32 = jnp.bfloat16, jnp.float32
    sem = pltpu.SemaphoreType.DMA
    tile = (lines, lanes)
    scratch = [
        pltpu.VMEM((K, Z) + tile, bf),
        pltpu.VMEM((K, Y - 1, Z) + tile, bf),
        pltpu.VMEM((K, Z - 1) + tile, bf),
        pltpu.VMEM((K, Z - 1) + tile, bf),
        pltpu.VMEM((K, grp) + tile, bf),
        pltpu.VMEM((K,) + tile, f32),
        pltpu.VMEM((blocks, 8, lanes), f32),
        pltpu.VMEM((blocks, 8, lanes), f32),
        pltpu.VMEM((8, lanes), f32),
        pltpu.VMEM((dp - 1, 8, lanes), f32),
        pltpu.VMEM((8, lanes), f32),
        pltpu.VMEM((grp - 1, 8, lanes), f32),
        sem((K,)),
        sem((K, Y - 1)), sem((K, Y - 1)),
        sem((K, Z - 1)), sem((K, Z - 1)),
        sem((K, grp - 1)), sem((K, grp - 1)),
        sem((dp - 1,)), sem((dp - 1,)),
        sem((grp - 1,)), sem((grp - 1,)),
    ]
    mean, top = pl.pallas_call(
        functools.partial(kernel, cfg),
        out_shape=(
            jax.ShapeDtypeStruct((K,) + tile, bf),
            jax.ShapeDtypeStruct((8, lanes), bf),
        ),
        in_specs=[
            pl.BlockSpec(memory_space=pltpu.SMEM),
            pl.BlockSpec(memory_space=pltpu.SMEM),
            pl.BlockSpec(memory_space=pltpu.HBM),
        ],
        out_specs=(
            pl.BlockSpec(memory_space=pltpu.VMEM),
            pl.BlockSpec(memory_space=pltpu.VMEM),
        ),
        scratch_shapes=scratch,
        compiler_params=pltpu.CompilerParams(collective_id=0, has_side_effects=True),
    )(block_len, amax_history, gradients.reshape((Z, Y, K) + tile))
    return mean.reshape(rows // dp, lanes), top[0, :blocks]


def solution(mesh):
    placed = (P("grp", "dp", None, None), P(), P())
    return jax.shard_map(
        body, mesh=mesh, in_specs=placed, out_specs=(P("dp", None), P()), check_vma=False
    )
```

```python
import functools

import jax
import jax.numpy as jnp
from jax import lax
from jax.experimental import pallas as pl
from jax.experimental.pallas import tpu as pltpu
from jax.sharding import PartitionSpec as P

SATURATE = 448.0
CHUNKS = 16
Z_FIRST = 3
STEP = 1
MESH = pl.DeviceIdType.MESH


def y_extent(dp):
    y = 1
    while (2 * y) * (2 * y) <= dp:
        y *= 2
    return y


def kernel(
    cfg, len_ref, hist_ref, grad, out, amax_out,
    own, ybuf, zin, zout, own_b, zin_b, zout_b, mout_b, yin_b,
    qbuf, scale_buf, svec, acc, msg, maxima,
    own_sem, y_send, y_recv, z_send, z_recv, q_send, q_recv,
    ob_sem, yb_send, yb_recv, zb_send, zb_recv, m_send, m_recv,
):
    dp, grp, Y, Z, K, NB, lines, piece = cfg
    NA = K - NB
    blocks = len_ref.shape[0]
    hist = hist_ref.shape[0]
    devices = dp * grp
    d = lax.axis_index("dp")
    g = lax.axis_index("grp")
    z, y = d // Y, d % Y
    base = d * (K * lines)

    def copy(src, dst, send, recv, target):
        return pltpu.make_async_remote_copy(
            src_ref=src, dst_ref=dst, send_sem=send, recv_sem=recv,
            device_id=target, device_id_type=MESH,
        )

    def own_copy(a):
        return pltpu.make_async_copy(grad.at[:, y, NB + a], own.at[a], own_sem.at[a])

    def own_b_copy(b):
        return pltpu.make_async_copy(grad.at[:, :, b], own_b.at[b], ob_sem.at[b])

    def y_copy(a, j):
        peer = (y + j) % Y
        return copy(grad.at[:, peer, NB + a], ybuf.at[a, j - 1], y_send.at[a, j - 1],
                    y_recv.at[a, j - 1], {"dp": z * Y + peer})

    def yb_copy(b, j):
        peer = (y + j) % Y
        return copy(mout_b.at[b, j - 1], yin_b.at[b, j - 1], yb_send.at[b, j - 1],
                    yb_recv.at[b, j - 1], {"dp": z * Y + peer})

    chain_a = (zin, zout, z_send, z_recv)
    chain_b = (zin_b, zout_b, zb_send, zb_recv)

    def hop(chain, i, way, t):
        into, outof, send, recv = chain
        return copy(outof.at[i, t], into.at[i, way, t], send.at[i, t], recv.at[i, way, t],
                    {"dp": (z + 1 - 2 * way) * Y + y})

    def arrival(chain, i, way, t):
        into, outof, send, recv = chain
        return copy(into.at[i, way, t], into.at[i, way, t], send.at[i, t], recv.at[i, way, t],
                    {"dp": (z - 1 + 2 * way) * Y + y})

    def await_hop(chain, i, way, t):
        @pl.when(z > 0 if way == 0 else z < Z - 1)
        def _():
            arrival(chain, i, way, t).wait_recv()

    def q_copy(k, j):
        return copy(qbuf.at[k, g], qbuf.at[k, g], q_send.at[k, j - 1], q_recv.at[k, j - 1],
                    {"grp": (g + j) % grp})

    def q_arrival(k, j):
        peer = (g + grp - j) % grp
        return copy(qbuf.at[k, peer], qbuf.at[k, peer], q_send.at[k, j - 1],
                    q_recv.at[k, j - 1], {"grp": peer})

    def device(j):
        flat = (d * grp + g + j) % devices
        return {"dp": flat // grp, "grp": flat % grp}

    def m_copy(j):
        return copy(msg, maxima.at[j - 1], m_send.at[j - 1], m_recv.at[j - 1], device(j))

    def every(action):
        def one(j, carry):
            action(j)
            return carry

        lax.fori_loop(1, devices, one, 0)

    barrier = pltpu.get_barrier_semaphore()
    every(lambda j: pl.semaphore_signal(
        barrier, inc=1, device_id=device(j), device_id_type=MESH))

    def each(count, action):
        def one(i, carry):
            action(i)
            return carry

        lax.fori_loop(0, count, one, 0)

    def upto(limit, action):
        for i in range(Z - 1):
            pl.when(limit > i)(functools.partial(action, i))

    each(NB, lambda b: own_b_copy(b).start())
    each(NA, lambda a: own_copy(a).start())
    for way, end in ((0, 0), (1, Z - 1)):
        @pl.when(z == end)
        def _(way=way):
            def clear(chain):
                into = chain[0]

                def one(i):
                    into[i, way] = jnp.zeros(into.shape[2:], into.dtype)

                return one

            each(NA, clear(chain_a))
            each(NB, clear(chain_b))
    ends = []
    total = jnp.int32(0)
    for c in range(blocks):
        total = total + len_ref[c]
        ends.append(total)
        top = jnp.full((8, 128), hist_ref[0, c], jnp.float32)
        for h in range(1, hist):
            top = jnp.maximum(top, jnp.full((8, 128), hist_ref[h, c], jnp.float32))
        svec[c] = SATURATE / jnp.maximum(top, 1.0)
    acc[...] = jnp.zeros(acc.shape, jnp.float32)
    pl.semaphore_wait(barrier, devices - 1)

    def send_y(a):
        for j in range(1, Y):
            y_copy(a, j).start()

    each(NA, send_y)

    def term_a(a, t):
        value = own[a, t].astype(jnp.float32)
        for i in range(Y - 1):
            value = value + ybuf[a, i, t].astype(jnp.float32)
        return value

    def term_b(b, t):
        return own_b[b, t].astype(jnp.float32)

    def stage_y(a):
        own_copy(a).wait()
        for j in range(1, Y):
            y_copy(a, j).wait_recv()

    def pass_on(chain, term, i, way):
        def one(s):
            t = Z - 1 - s if way == 0 else s
            await_hop(chain, i, way, t)
            value = term(i, t) + chain[0][i, way, t].astype(jnp.float32)
            chain[1][i, t] = value.astype(jnp.bfloat16)
            hop(chain, i, way, t).start()

        upto(Z - 1 - z if way == 0 else z, one)

    def merge_b(b):
        for way in range(2):
            await_hop(chain_b, b, way, z)
        for j in range(1, Y):
            peer = (y + j) % Y
            value = own_b[b, z, peer].astype(jnp.float32)
            for way in range(2):
                value = value + zin_b[b, way, z, peer].astype(jnp.float32)
            mout_b[b, j - 1] = value.astype(jnp.bfloat16)
            yb_copy(b, j).start()

    def q_a(a):
        for way in range(2):
            await_hop(chain_a, a, way, z)

        def total(rows):
            value = own[a, z, rows].astype(jnp.float32)
            for i in range(Y - 1):
                value = value + ybuf[a, i, z, rows].astype(jnp.float32)
            for way in range(2):
                value = value + zin[a, way, z, rows].astype(jnp.float32)
            return value

        stage_q(NB + a, total)

    def q_b(b):
        for j in range(1, Y):
            yb_copy(b, j).wait_recv()

        def total(rows):
            value = own_b[b, z, y, rows].astype(jnp.float32)
            for way in range(2):
                value = value + zin_b[b, way, z, y, rows].astype(jnp.float32)
            for i in range(Y - 1):
                value = value + yin_b[b, i, rows].astype(jnp.float32)
            return value

        stage_q(b, total)

    def stage_q(k, total):
        def step(i, tops):
            rows = pl.ds(pl.multiple_of(i * piece, piece), piece)
            value = total(rows)
            value = value.reshape(piece // 8, 8, 128)
            shape = value.shape
            first = (base + k * lines + i * piece) * 128
            place = (
                lax.broadcasted_iota(jnp.int32, shape, 0) * 1024
                + lax.broadcasted_iota(jnp.int32, shape, 1) * 128
                + lax.broadcasted_iota(jnp.int32, shape, 2)
            ) + first
            size = jnp.abs(value)
            scale = jnp.broadcast_to(svec[0][None], shape)
            below = place < ends[0]
            new = [jnp.maximum(tops[0], jnp.max(jnp.where(below, size, 0.0), axis=0))]
            for c in range(1, blocks):
                after = place >= ends[c - 1]
                scale = jnp.where(after, svec[c][None], scale)
                inside = after & (place < ends[c])
                new.append(jnp.maximum(tops[c], jnp.max(jnp.where(inside, size, 0.0), axis=0)))
            scale_buf[k, rows] = scale.reshape(piece, 128)
            quant = jnp.clip(value * scale, -SATURATE, SATURATE)
            qbuf[k, g, rows] = quant.reshape(piece, 128).astype(jnp.bfloat16)
            return tuple(new)

        tops = lax.fori_loop(0, lines // piece, step, tuple(acc[c] for c in range(blocks)))
        for c in range(blocks):
            acc[c] = tops[c]
        for j in range(1, grp):
            q_copy(k, j).start()

    def stage_max():
        top = jnp.max(acc[...], axis=1)
        top = jnp.max(top, axis=1, keepdims=True)
        lane = lax.broadcasted_iota(jnp.int32, (blocks, 128), 1)
        row = lax.broadcasted_iota(jnp.int32, (blocks, 128), 0)
        flat = jnp.max(jnp.where(lane == row, top, 0.0), axis=0, keepdims=True)
        msg[...] = flat
        every(lambda j: m_copy(j).start())

    def stage_out(k):
        for j in range(1, grp):
            q_arrival(k, j).wait_recv()
        value = qbuf[k, 0].astype(jnp.float32)
        for a in range(1, grp):
            value = value + qbuf[k, a].astype(jnp.float32)
        out[k] = (value / scale_buf[k] / (dp * grp)).astype(jnp.bfloat16)

    reach = STEP * (Z - 1)
    last = K + reach
    stages = (
        (lambda b: own_b_copy(b).wait(), NB, 0),
        (lambda b: pass_on(chain_b, term_b, b, 0), NB, STEP * z),
        (lambda b: pass_on(chain_b, term_b, b, 1), NB, STEP * (Z - 1 - z)),
        (merge_b, NB, reach + 1),
        (stage_y, NA, NB),
        (lambda a: pass_on(chain_a, term_a, a, 0), NA, NB + STEP * z),
        (lambda a: pass_on(chain_a, term_a, a, 1), NA, NB + STEP * (Z - 1 - z)),
        (q_b, NB, K),
        (q_a, NA, NB + reach + 1),
        (lambda b: stage_out(b), NB, K + 2),
        (lambda a: stage_out(NB + a), NA, NB + reach + 3),
    )

    def tick(t, carry):
        for stage, count, delay in stages:
            @pl.when((t >= delay) & (t < count + delay))
            def _(stage=stage, delay=delay):
                stage(t - delay)

            if stage is q_a:
                @pl.when(t == last)
                def _():
                    stage_max()
        return carry

    lax.fori_loop(0, K + reach + 3, tick, 0)

    every(lambda j: m_copy(j).wait_recv())
    top = jnp.maximum(jnp.max(maxima[...], axis=0), msg[...])
    amax_out[...] = jnp.broadcast_to(top, amax_out.shape).astype(jnp.bfloat16)

    def finish_a(a):
        for j in range(1, Y):
            y_copy(a, j).wait_send()
        upto(Z - 1 - z, lambda s: hop(chain_a, a, 0, Z - 1 - s).wait_send())
        upto(z, lambda s: hop(chain_a, a, 1, s).wait_send())

    def finish_b(b):
        for j in range(1, Y):
            yb_copy(b, j).wait_send()
        upto(Z - 1 - z, lambda s: hop(chain_b, b, 0, Z - 1 - s).wait_send())
        upto(z, lambda s: hop(chain_b, b, 1, s).wait_send())

    def finish(k):
        for j in range(1, grp):
            q_copy(k, j).wait_send()

    each(NA, finish_a)
    each(NB, finish_b)
    each(K, finish)
    every(lambda j: m_copy(j).wait_send())


def body(gradients, block_len, amax_history):
    dp = lax.axis_size("dp")
    grp = lax.axis_size("grp")
    rows, lanes = gradients.shape[2:]
    Y = y_extent(dp)
    Z = dp // Y
    K = min(CHUNKS, rows // dp // 32)
    NB = min(Z_FIRST, K - 1)
    NA = K - NB
    lines = rows // dp // K
    piece = 32
    blocks = block_len.shape[0]
    cfg = (dp, grp, Y, Z, K, NB, lines, piece)
    bf, f32 = jnp.bfloat16, jnp.float32
    sem = pltpu.SemaphoreType.DMA
    tile = (lines, lanes)
    scratch = [
        pltpu.VMEM((NA, Z) + tile, bf),
        pltpu.VMEM((NA, Y - 1, Z) + tile, bf),
        pltpu.VMEM((NA, 2, Z) + tile, bf),
        pltpu.VMEM((NA, Z) + tile, bf),
        pltpu.VMEM((NB, Z, Y) + tile, bf),
        pltpu.VMEM((NB, 2, Z, Y) + tile, bf),
        pltpu.VMEM((NB, Z, Y) + tile, bf),
        pltpu.VMEM((NB, Y - 1) + tile, bf),
        pltpu.VMEM((NB, Y - 1) + tile, bf),
        pltpu.VMEM((K, grp) + tile, bf),
        pltpu.VMEM((K,) + tile, f32),
        pltpu.VMEM((blocks, 8, lanes), f32),
        pltpu.VMEM((blocks, 8, lanes), f32),
        pltpu.VMEM((1, lanes), f32),
        pltpu.VMEM((dp * grp - 1, 1, lanes), f32),
        sem((NA,)),
        sem((NA, Y - 1)), sem((NA, Y - 1)),
        sem((NA, Z)), sem((NA, 2, Z)),
        sem((K, grp - 1)), sem((K, grp - 1)),
        sem((NB,)),
        sem((NB, Y - 1)), sem((NB, Y - 1)),
        sem((NB, Z)), sem((NB, 2, Z)),
        sem((dp * grp - 1,)), sem((dp * grp - 1,)),
    ]
    mean, top = pl.pallas_call(
        functools.partial(kernel, cfg),
        out_shape=(
            jax.ShapeDtypeStruct((K,) + tile, bf),
            jax.ShapeDtypeStruct((8, lanes), bf),
        ),
        in_specs=[
            pl.BlockSpec(memory_space=pltpu.SMEM),
            pl.BlockSpec(memory_space=pltpu.SMEM),
            pl.BlockSpec(memory_space=pltpu.HBM),
        ],
        out_specs=(
            pl.BlockSpec(memory_space=pltpu.VMEM),
            pl.BlockSpec(memory_space=pltpu.VMEM),
        ),
        scratch_shapes=scratch,
        compiler_params=pltpu.CompilerParams(collective_id=0, has_side_effects=True),
    )(block_len, amax_history, gradients.reshape((Z, Y, K) + tile))
    return mean.reshape(rows // dp, lanes), top[0, :blocks]


def solution(mesh):
    placed = (P("grp", "dp", None, None), P(), P())
    return jax.shard_map(
        body, mesh=mesh, in_specs=placed, out_specs=(P("dp", None), P()), check_vma=False
    )
```

```python
import functools

import jax
import jax.numpy as jnp
from jax import lax
from jax.experimental import pallas as pl
from jax.experimental.pallas import tpu as pltpu
from jax.sharding import PartitionSpec as P

SATURATE = 448.0
CHUNKS = 16
Z_FIRST = 3
STEP = 1
MESH = pl.DeviceIdType.MESH


def y_extent(dp):
    y = 1
    while (2 * y) * (2 * y) <= dp:
        y *= 2
    return y


def kernel(
    cfg, len_ref, hist_ref, grad, out, amax_out,
    own, ybuf, zin, zout, own_b, zin_b, zout_b, mout_b, yin_b,
    qbuf, scale_buf, svec, acc, msg, maxima,
    own_sem, y_send, y_recv, z_send, z_recv, q_send, q_recv,
    ob_sem, yb_send, yb_recv, zb_send, zb_recv, m_send, m_recv,
):
    dp, grp, Y, Z, K, NB, lines, piece = cfg
    NA = K - NB
    blocks = len_ref.shape[0]
    hist = hist_ref.shape[0]
    devices = dp * grp
    d = lax.axis_index("dp")
    g = lax.axis_index("grp")
    z, y = d // Y, d % Y
    base = d * (K * lines)

    def copy(src, dst, send, recv, target):
        return pltpu.make_async_remote_copy(
            src_ref=src, dst_ref=dst, send_sem=send, recv_sem=recv,
            device_id=target, device_id_type=MESH,
        )

    def own_copy(a):
        return pltpu.make_async_copy(grad.at[:, y, NB + a], own.at[a], own_sem.at[a])

    def own_b_copy(b):
        return pltpu.make_async_copy(grad.at[:, :, b], own_b.at[b], ob_sem.at[b])

    def y_copy(a, j):
        peer = (y + j) % Y
        return copy(grad.at[:, peer, NB + a], ybuf.at[a, j - 1], y_send.at[a, j - 1],
                    y_recv.at[a, j - 1], {"dp": z * Y + peer})

    def yb_copy(b, j):
        peer = (y + j) % Y
        return copy(mout_b.at[b, j - 1], yin_b.at[b, j - 1], yb_send.at[b, j - 1],
                    yb_recv.at[b, j - 1], {"dp": z * Y + peer})

    chain_a = (zin, zout, z_send, z_recv)
    chain_b = (zin_b, zout_b, zb_send, zb_recv)

    def hop(chain, i, way, t):
        into, outof, send, recv = chain
        return copy(outof.at[i, t], into.at[i, way, t], send.at[i, t], recv.at[i, way, t],
                    {"dp": (z + 1 - 2 * way) * Y + y})

    def arrival(chain, i, way, t):
        into, outof, send, recv = chain
        return copy(into.at[i, way, t], into.at[i, way, t], send.at[i, t], recv.at[i, way, t],
                    {"dp": (z - 1 + 2 * way) * Y + y})

    def await_hop(chain, i, way, t):
        @pl.when(z > 0 if way == 0 else z < Z - 1)
        def _():
            arrival(chain, i, way, t).wait_recv()

    def q_copy(k, j):
        return copy(qbuf.at[k, g], qbuf.at[k, g], q_send.at[k, j - 1], q_recv.at[k, j - 1],
                    {"grp": (g + j) % grp})

    def q_arrival(k, j):
        peer = (g + grp - j) % grp
        return copy(qbuf.at[k, peer], qbuf.at[k, peer], q_send.at[k, j - 1],
                    q_recv.at[k, j - 1], {"grp": peer})

    def device(j):
        flat = (d * grp + g + j) % devices
        return {"dp": flat // grp, "grp": flat % grp}

    def m_copy(j):
        return copy(msg, maxima.at[j - 1], m_send.at[j - 1], m_recv.at[j - 1], device(j))

    def every(action):
        def one(j, carry):
            action(j)
            return carry

        lax.fori_loop(1, devices, one, 0)

    barrier = pltpu.get_barrier_semaphore()
    every(lambda j: pl.semaphore_signal(
        barrier, inc=1, device_id=device(j), device_id_type=MESH))

    def each(count, action):
        def one(i, carry):
            action(i)
            return carry

        lax.fori_loop(0, count, one, 0)

    def upto(limit, action):
        for i in range(Z - 1):
            pl.when(limit > i)(functools.partial(action, i))

    each(NB, lambda b: own_b_copy(b).start())
    each(NA, lambda a: own_copy(a).start())
    for way, end in ((0, 0), (1, Z - 1)):
        @pl.when(z == end)
        def _(way=way):
            def clear(chain):
                into = chain[0]

                def one(i):
                    into[i, way] = jnp.zeros(into.shape[2:], into.dtype)

                return one

            each(NA, clear(chain_a))
            each(NB, clear(chain_b))
    ends = []
    total = jnp.int32(0)
    for c in range(blocks):
        total = total + len_ref[c]
        ends.append(total)
        top = jnp.full((8, 128), hist_ref[0, c], jnp.float32)
        for h in range(1, hist):
            top = jnp.maximum(top, jnp.full((8, 128), hist_ref[h, c], jnp.float32))
        svec[c] = SATURATE / jnp.maximum(top, 1.0)
    acc[...] = jnp.zeros(acc.shape, jnp.float32)
    pl.semaphore_wait(barrier, devices - 1)

    def send_y(a):
        for j in range(1, Y):
            y_copy(a, j).start()

    each(NA, send_y)

    def term_a(a, t):
        value = own[a, t].astype(jnp.float32)
        for i in range(Y - 1):
            value = value + ybuf[a, i, t].astype(jnp.float32)
        return value

    def term_b(b, t):
        return own_b[b, t].astype(jnp.float32)

    def stage_y(a):
        own_copy(a).wait()
        for j in range(1, Y):
            y_copy(a, j).wait_recv()

    def pass_on(chain, term, i, way):
        def one(s):
            t = Z - 1 - s if way == 0 else s
            await_hop(chain, i, way, t)
            value = term(i, t) + chain[0][i, way, t].astype(jnp.float32)
            chain[1][i, t] = value.astype(jnp.bfloat16)
            hop(chain, i, way, t).start()

        upto(Z - 1 - z if way == 0 else z, one)

    def merge_b(b):
        for way in range(2):
            await_hop(chain_b, b, way, z)
        for j in range(1, Y):
            peer = (y + j) % Y
            value = own_b[b, z, peer].astype(jnp.float32)
            for way in range(2):
                value = value + zin_b[b, way, z, peer].astype(jnp.float32)
            mout_b[b, j - 1] = value.astype(jnp.bfloat16)
            yb_copy(b, j).start()

    def q_a(a):
        for way in range(2):
            await_hop(chain_a, a, way, z)

        def total(rows):
            value = own[a, z, rows].astype(jnp.float32)
            for i in range(Y - 1):
                value = value + ybuf[a, i, z, rows].astype(jnp.float32)
            for way in range(2):
                value = value + zin[a, way, z, rows].astype(jnp.float32)
            return value

        stage_q(NB + a, total)

    def q_b(b):
        for j in range(1, Y):
            yb_copy(b, j).wait_recv()

        def total(rows):
            value = own_b[b, z, y, rows].astype(jnp.float32)
            for way in range(2):
                value = value + zin_b[b, way, z, y, rows].astype(jnp.float32)
            for i in range(Y - 1):
                value = value + yin_b[b, i, rows].astype(jnp.float32)
            return value

        stage_q(b, total)

    def stage_q(k, total):
        def step(i, tops):
            rows = pl.ds(pl.multiple_of(i * piece, piece), piece)
            value = total(rows)
            value = value.reshape(piece // 8, 8, 128)
            shape = value.shape
            first = (base + k * lines + i * piece) * 128
            place = (
                lax.broadcasted_iota(jnp.int32, shape, 0) * 1024
                + lax.broadcasted_iota(jnp.int32, shape, 1) * 128
                + lax.broadcasted_iota(jnp.int32, shape, 2)
            ) + first
            size = jnp.abs(value)
            scale = jnp.broadcast_to(svec[0][None], shape)
            below = place < ends[0]
            new = [jnp.maximum(tops[0], jnp.max(jnp.where(below, size, 0.0), axis=0))]
            for c in range(1, blocks):
                after = place >= ends[c - 1]
                scale = jnp.where(after, svec[c][None], scale)
                inside = after & (place < ends[c])
                new.append(jnp.maximum(tops[c], jnp.max(jnp.where(inside, size, 0.0), axis=0)))
            scale_buf[k, rows] = scale.reshape(piece, 128)
            quant = jnp.clip(value * scale, -SATURATE, SATURATE)
            qbuf[k, g, rows] = quant.reshape(piece, 128).astype(jnp.bfloat16)
            return tuple(new)

        tops = lax.fori_loop(0, lines // piece, step, tuple(acc[c] for c in range(blocks)))
        for c in range(blocks):
            acc[c] = tops[c]
        for j in range(1, grp):
            q_copy(k, j).start()

    def stage_max():
        top = jnp.max(acc[...], axis=1)
        top = jnp.max(top, axis=1, keepdims=True)
        lane = lax.broadcasted_iota(jnp.int32, (blocks, 128), 1)
        row = lax.broadcasted_iota(jnp.int32, (blocks, 128), 0)
        flat = jnp.max(jnp.where(lane == row, top, 0.0), axis=0, keepdims=True)
        msg[...] = flat
        every(lambda j: m_copy(j).start())

    def stage_out(k):
        for j in range(1, grp):
            q_arrival(k, j).wait_recv()
        value = qbuf[k, 0].astype(jnp.float32)
        for a in range(1, grp):
            value = value + qbuf[k, a].astype(jnp.float32)
        out[k] = (value / scale_buf[k] / (dp * grp)).astype(jnp.bfloat16)

    reach = STEP * (Z - 1)
    last = K + reach
    stages = (
        (lambda b: own_b_copy(b).wait(), NB, 0),
        (lambda b: pass_on(chain_b, term_b, b, 0), NB, STEP * z),
        (lambda b: pass_on(chain_b, term_b, b, 1), NB, STEP * (Z - 1 - z)),
        (merge_b, NB, reach + 1),
        (stage_y, NA, NB),
        (lambda a: pass_on(chain_a, term_a, a, 0), NA, NB + STEP * z),
        (lambda a: pass_on(chain_a, term_a, a, 1), NA, NB + STEP * (Z - 1 - z)),
        (q_b, NB, K),
        (q_a, NA, NB + reach + 1),
        (lambda b: stage_out(b), NB, K + 3),
        (lambda a: stage_out(NB + a), NA, NB + reach + 4),
    )

    def tick(t, carry):
        for stage, count, delay in stages:
            @pl.when((t >= delay) & (t < count + delay))
            def _(stage=stage, delay=delay):
                stage(t - delay)

            if stage is q_a:
                @pl.when(t == last)
                def _():
                    stage_max()
        return carry

    lax.fori_loop(0, K + reach + 4, tick, 0)

    every(lambda j: m_copy(j).wait_recv())
    top = jnp.maximum(jnp.max(maxima[...], axis=0), msg[...])
    amax_out[...] = jnp.broadcast_to(top, amax_out.shape).astype(jnp.bfloat16)

    def finish_a(a):
        for j in range(1, Y):
            y_copy(a, j).wait_send()
        upto(Z - 1 - z, lambda s: hop(chain_a, a, 0, Z - 1 - s).wait_send())
        upto(z, lambda s: hop(chain_a, a, 1, s).wait_send())

    def finish_b(b):
        for j in range(1, Y):
            yb_copy(b, j).wait_send()
        upto(Z - 1 - z, lambda s: hop(chain_b, b, 0, Z - 1 - s).wait_send())
        upto(z, lambda s: hop(chain_b, b, 1, s).wait_send())

    def finish(k):
        for j in range(1, grp):
            q_copy(k, j).wait_send()

    each(NA, finish_a)
    each(NB, finish_b)
    each(K, finish)
    every(lambda j: m_copy(j).wait_send())


def body(gradients, block_len, amax_history):
    dp = lax.axis_size("dp")
    grp = lax.axis_size("grp")
    rows, lanes = gradients.shape[2:]
    Y = y_extent(dp)
    Z = dp // Y
    K = min(CHUNKS, rows // dp // 32)
    NB = min(Z_FIRST, K - 1)
    NA = K - NB
    lines = rows // dp // K
    piece = 32
    blocks = block_len.shape[0]
    cfg = (dp, grp, Y, Z, K, NB, lines, piece)
    bf, f32 = jnp.bfloat16, jnp.float32
    sem = pltpu.SemaphoreType.DMA
    tile = (lines, lanes)
    scratch = [
        pltpu.VMEM((NA, Z) + tile, bf),
        pltpu.VMEM((NA, Y - 1, Z) + tile, bf),
        pltpu.VMEM((NA, 2, Z) + tile, bf),
        pltpu.VMEM((NA, Z) + tile, bf),
        pltpu.VMEM((NB, Z, Y) + tile, bf),
        pltpu.VMEM((NB, 2, Z, Y) + tile, bf),
        pltpu.VMEM((NB, Z, Y) + tile, bf),
        pltpu.VMEM((NB, Y - 1) + tile, bf),
        pltpu.VMEM((NB, Y - 1) + tile, bf),
        pltpu.VMEM((K, grp) + tile, bf),
        pltpu.VMEM((K,) + tile, f32),
        pltpu.VMEM((blocks, 8, lanes), f32),
        pltpu.VMEM((blocks, 8, lanes), f32),
        pltpu.VMEM((1, lanes), f32),
        pltpu.VMEM((dp * grp - 1, 1, lanes), f32),
        sem((NA,)),
        sem((NA, Y - 1)), sem((NA, Y - 1)),
        sem((NA, Z)), sem((NA, 2, Z)),
        sem((K, grp - 1)), sem((K, grp - 1)),
        sem((NB,)),
        sem((NB, Y - 1)), sem((NB, Y - 1)),
        sem((NB, Z)), sem((NB, 2, Z)),
        sem((dp * grp - 1,)), sem((dp * grp - 1,)),
    ]
    mean, top = pl.pallas_call(
        functools.partial(kernel, cfg),
        out_shape=(
            jax.ShapeDtypeStruct((K,) + tile, bf),
            jax.ShapeDtypeStruct((8, lanes), bf),
        ),
        in_specs=[
            pl.BlockSpec(memory_space=pltpu.SMEM),
            pl.BlockSpec(memory_space=pltpu.SMEM),
            pl.BlockSpec(memory_space=pltpu.HBM),
        ],
        out_specs=(
            pl.BlockSpec(memory_space=pltpu.VMEM),
            pl.BlockSpec(memory_space=pltpu.VMEM),
        ),
        scratch_shapes=scratch,
        compiler_params=pltpu.CompilerParams(collective_id=0, has_side_effects=True),
    )(block_len, amax_history, gradients.reshape((Z, Y, K) + tile))
    return mean.reshape(rows // dp, lanes), top[0, :blocks]


def solution(mesh):
    placed = (P("grp", "dp", None, None), P(), P())
    return jax.shard_map(
        body, mesh=mesh, in_specs=placed, out_specs=(P("dp", None), P()), check_vma=False
    )
```
